16 devices in a mesh: rep: 1, r: 4 (over y, z), s: 4 (over x, core).
Axes of the slice: x: 2, y: 2, z: 2, core: 2. Of those that a mesh axis runs over, the one named last changes fastest.
Arguments:
- x: bfloat16 [16, 4096, 640], P(('rep', 'r', 's'))
- dy: bfloat16 [16, 4096, 640], P(('rep', 'r', 's'))
- w_gate: bfloat16 [2, 640, 2048], P(None, 's')
- w_up: bfloat16 [2, 640, 2048], P(None, 's')
- w_down: bfloat16 [2, 2048, 640], P(None, 's')
- m_w_gate: float32 [2, 640, 2048], P(None, 's')
- m_w_up: float32 [2, 640, 2048], P(None, 's')
- m_w_down: float32 [2, 2048, 640], P(None, 's')
- v_w_gate: float32 [2, 640, 2048], P(None, 's')
- v_w_up: float32 [2, 640, 2048], P(None, 's')
- v_w_down: float32 [2, 2048, 640], P(None, 's')
Outputs:
- output 1: bfloat16 [2, 640, 2048], P('rep', 's')
- output 2: bfloat16 [2, 640, 2048], P('rep', 's')
- output 3: bfloat16 [2, 2048, 640], P('rep', 's')
- output 4: float32 [2, 640, 2048], P('rep', 's')
- output 5: float32 [2, 640, 2048], P('rep', 's')
- output 6: float32 [2, 2048, 640], P('rep', 's')
- output 7: float32 [2, 640, 2048], P('rep', 's')
- output 8: float32 [2, 640, 2048], P('rep', 's')
- output 9: float32 [2, 2048, 640], P('rep', 's')
All inputs are finite; a program needn't handle non-finite values.
Results may differ from the reference program's by a relative error of at most 0.022.
Values are sent between devices in bfloat16 or wider.
A program may use at most 2 GiB of HBM per device.

```python
import jax
import jax.numpy as jnp
from jax import lax

SEQUENCES = 16
TOKENS = 4096
D = 640
FF = 2048
LAYERS = 2
NAMES = ("w_gate", "w_up", "w_down")
SHAPES = {"w_gate": (LAYERS, D, FF), "w_up": (LAYERS, D, FF), "w_down": (LAYERS, FF, D)}


def bump(key, n, height):
    away = (jnp.arange(n, dtype=jnp.int32) - jax.random.randint(key, (), 0, n, jnp.int32)) % n
    return jnp.where(away < n // 8, height, 1.0)


def together(key, own, strength):
    shared = jax.random.normal(key, own.shape[1:], jnp.float32)
    return (own + strength * shared) * lax.rsqrt(1 + strength * strength)


def setup_inputs(seed: int = 0, part: int = 0) -> dict:
    kx, kdy, ka, kb, kz, kf, kh, kl, *keys = jax.random.split(jax.random.key(seed), 8 + 3 * len(NAMES))
    kx, kdy, ka, kb = (jax.random.fold_in(k, part) for k in (kx, kdy, ka, kb))
    kw, km, kv = (keys[i::3] for i in range(3))
    shape = (SEQUENCES, TOKENS, D)
    much_x, much_dy = jax.random.uniform(kz, (2,), jnp.float32, 0.0, 1.0)
    loud = 2.0 ** jax.random.uniform(jax.random.fold_in(kz, 1), (), jnp.float32, -1.0, 2.0)
    layers = 2.0 ** jax.random.uniform(kl, (LAYERS, 1, 1), jnp.float32, -1.0, 1.0)
    x = together(ka, jax.random.normal(kx, shape, jnp.float32), much_x) * bump(kf, D, 4.0)
    dy = together(kb, jax.random.normal(kdy, shape, jnp.float32), much_dy)
    drawn = {"x": x.astype(jnp.bfloat16), "dy": (loud * dy * (SEQUENCES * TOKENS) ** -0.5).astype(jnp.bfloat16)}
    for key, name in zip(kw, NAMES, strict=True):
        w = jax.random.normal(key, SHAPES[name], jnp.float32) * SHAPES[name][1] ** -0.5
        drawn[name] = (w * {"w_gate": 1.0, "w_up": bump(kh, FF, 4.0), "w_down": layers}[name]).astype(jnp.bfloat16)
    for key, name in zip(km, NAMES, strict=True):
        drawn[f"m_{name}"] = 0.1 * jax.random.normal(key, SHAPES[name], jnp.float32)
    for key, name in zip(kv, NAMES, strict=True):
        drawn[f"v_{name}"] = jax.random.uniform(key, SHAPES[name], jnp.float32, 0.005, 0.015)
    return drawn


def matmul(a, w):
    return jnp.dot(a, w, preferred_element_type=jnp.float32).astype(jnp.bfloat16)


def normed(h):
    wide = h.astype(jnp.float32)
    scale = lax.rsqrt(jnp.mean(wide**2, -1, keepdims=True) + 1e-6)
    return (wide * scale).astype(jnp.bfloat16)


def layer(h, w):
    a = normed(h)
    gate = jnp.dot(a, w["w_gate"], preferred_element_type=jnp.float32)
    up = jnp.dot(a, w["w_up"], preferred_element_type=jnp.float32)
    return h + matmul((jax.nn.silu(gate) * up).astype(jnp.bfloat16), w["w_down"])


def adamw(w, m, v, g):
    m = 0.9 * m + 0.1 * g
    v = 0.95 * v + 0.05 * g * g
    step = m * lax.rsqrt(v + 1e-8) + 0.1 * w
    return (w - 0.02 * step).astype(jnp.bfloat16), m, v


def clipped(gradients, sum_of_squares, count):
    factor = jnp.minimum(1.0, 0.5 * lax.rsqrt(sum_of_squares / count + 1e-30))
    return [g * factor for g in gradients]


def stack(weights, h):
    return lax.scan(lambda h, w: (layer(h, w), None), h, weights)[0]


def reference(x, dy, w_gate, w_up, w_down, m_w_gate, m_w_up, m_w_down, v_w_gate, v_w_up, v_w_down):
    weights = dict(zip(NAMES, (w_gate, w_up, w_down), strict=True))

    def take(so_far, sequence):
        h, by_y = sequence
        _, back = jax.vjp(lambda w: stack(w, h), weights)
        return jax.tree.map(lambda total, term: total + term.astype(jnp.float32), so_far, back(by_y)[0]), None

    none_yet = {name: jnp.zeros(w.shape, jnp.float32) for name, w in weights.items()}
    by_weights, _ = lax.scan(take, none_yet, (x, dy))
    gradients = [by_weights[name].astype(jnp.bfloat16).astype(jnp.float32) for name in NAMES]
    gradients = clipped(gradients, sum(jnp.sum(g * g) for g in gradients), sum(g.size for g in gradients))
    new = [
        adamw(w.astype(jnp.float32), m, v, g)
        for w, m, v, g in zip((w_gate, w_up, w_down), (m_w_gate, m_w_up, m_w_down), (v_w_gate, v_w_up, v_w_down), gradients, strict=True)
    ]
    return tuple(one[which] for which in range(3) for one in new)
```

```python
import jax
import jax.numpy as jnp
from jax import lax
from jax.experimental import pallas as pl
from jax.experimental.pallas import tpu as pltpu
from jax.sharding import PartitionSpec as P

D, FF, TOK = 640, 2048, 4096
C, F, T = 4, 512, 1024
NT = TOK // T
STEPS = C * NT
RG, RD = 160, 128
EARLY = 6
f32, bf16 = jnp.float32, jnp.bfloat16
MESH = pl.DeviceIdType.MESH
VMEM = pl.BlockSpec(memory_space=pltpu.VMEM)
ANY = pl.BlockSpec(memory_space=pl.ANY)
DMA = pltpu.SemaphoreType.DMA


def dg(a, b, ca, cb):
    return lax.dot_general(a, b, (((ca,), (cb,)), ((), ())), preferred_element_type=f32)


def sigmoid(g):
    return 0.5 * jnp.tanh(0.5 * g) + 0.5


def tile(t):
    return pl.ds(pl.multiple_of(t * T, T), T)


def rows(s, n):
    return pl.ds(pl.multiple_of(s * n, n), n)


def scale_of(wide):
    return lax.rsqrt(jnp.mean(wide * wide, 0, keepdims=True) + 1e-6)


class Place:
    def __init__(self):
        r, self.s = lax.axis_index("r"), lax.axis_index("s")
        self.chip, self.k = self.s // 2, self.s % 2
        y, z = r // 2, r % 2
        self.x_s = 2 * (1 - self.chip) + self.k
        self.core = {"s": 2 * self.chip + 1 - self.k}
        self.x = {"s": self.x_s}
        self.diag = {"s": 2 * (1 - self.chip) + 1 - self.k}
        self.y = {"r": 2 * (1 - y) + z}
        self.z = {"r": 2 * y + 1 - z}


def greet(peers):
    barrier = pltpu.get_barrier_semaphore()
    for peer in peers:
        pl.semaphore_signal(barrier, inc=1, device_id=peer, device_id_type=MESH)
    pl.semaphore_wait(barrier, len(peers))


def remote(src, dst, send, recv, peer):
    return pltpu.make_async_remote_copy(
        src_ref=src, dst_ref=dst, send_sem=send, recv_sem=recv, device_id=peer, device_id_type=MESH
    )


class Gather:
    def __init__(self, at, full, shards, own, sems):
        self.at, self.full, self.shards, self.own, self.sems = at, full, shards, own, sems

    def slot(self, m, u, s):
        return self.full[m].at[u, rows(s, RG if m < 2 else RD), :]

    def fetch(self, u, layer, c):
        for m in range(3):
            if m < 2:
                for q in range(4):
                    pltpu.make_async_copy(
                        self.shards[m].at[layer, :, pl.ds(q * F + c * 128, 128)],
                        self.full[m].at[u, rows(self.at.s, RG), pl.ds(q * 128, 128)],
                        self.own.at[u, m],
                    ).start()
            else:
                pltpu.make_async_copy(self.shards[m].at[layer, pl.ds(c * RD, RD), :], self.slot(m, u, self.at.s), self.own.at[u, m]).start()

    def copy(self, kind, m, u):
        s = self.at.x_s if kind == 2 else self.at.s
        slot = self.slot(m, u, s)
        return remote(slot, slot, self.sems.at[0, kind, u, m], self.sems.at[1, kind, u, m], self.at.x if kind == 0 else self.at.core)

    def send(self, u):
        for m in range(3):
            slot = self.slot(m, u, self.at.s)
            pltpu.make_async_copy(slot, slot, self.own.at[u, m]).wait()
            self.copy(0, m, u).start()
            self.copy(1, m, u).start()

    def forward(self, u):
        for m in range(3):
            self.copy(0, m, u).wait_recv()
            self.copy(2, m, u).start()

    def ready(self, u):
        for m in range(3):
            self.copy(1, m, u).wait_recv()
            self.copy(2, m, u).wait_recv()

    def finish(self, u):
        for m in range(3):
            for kind in range(3):
                self.copy(kind, m, u).wait_send()


def gather_scratch(units):
    return [
        pltpu.VMEM((units, D, F), bf16),
        pltpu.VMEM((units, D, F), bf16),
        pltpu.VMEM((units, F, D), bf16),
        DMA((units, 3)),
        DMA((2, 3, units, 3)),
    ]


class Reduce:
    def __init__(self, at, acc, refs):
        self.at, self.acc = at, acc
        self.p, self.r1, self.b, self.r2, self.q, self.r3, self.q2, self.r4 = (refs[3 * i : 3 * i + 3] for i in range(8))
        self.ss, self.rs = refs[24:]

    def term(self, m, slot, s):
        if m < 2:
            return self.acc[m][slot, rows(s, RG), :]
        return self.acc[2][slot, :, rows(s, RD)].T

    def half(self, m, n):
        h = (RG if m < 2 else RD) // 2
        return pl.ds(n * h, h)

    def copies(self, stage, m, u):
        at = self.at
        if stage == 0:
            return [remote(self.p[m], self.r1[m].at[u], self.ss.at[0, m], self.rs.at[u, 0, m], at.core)]
        if stage == 1:
            return [remote(self.b[m], self.r2[m].at[u], self.ss.at[1, m], self.rs.at[u, 1, m], at.x)]
        src, dst, ways = (self.q, self.r3, (at.y, at.z)) if stage == 2 else (self.q2, self.r4, (at.z, at.y))
        return [
            remote(src[m].at[self.half(m, n)], dst[m].at[u, self.half(m, n)], self.ss.at[2 * stage - 2 + n, m], self.rs.at[u, 2 * stage - 2 + n, m], ways[n])
            for n in range(2)
        ]

    def start(self, stage, m, u):
        for copy in self.copies(stage, m, u):
            copy.start()

    def wait(self, stage, m, u):
        for copy in self.copies(stage, m, u):
            copy.wait()

    def to_core(self, u, slot):
        for m in range(3):
            for j in range(2):
                self.p[m][j] = self.term(m, slot, 2 * j + 1 - self.at.k).astype(bf16)
            self.start(0, m, u)

    def to_x(self, u, slot):
        at = self.at
        for m in range(3):
            self.wait(0, m, u)
            self.b[m][...] = (self.term(m, slot, at.x_s) + self.r1[m][u, 1 - at.chip].astype(f32)).astype(bf16)
            self.start(1, m, u)

    def to_yz(self, u, slot):
        at = self.at
        for m in range(3):
            self.wait(1, m, u)
            total = self.term(m, slot, at.s) + self.r1[m][u, at.chip].astype(f32) + self.r2[m][u].astype(f32)
            self.q[m][...] = total.astype(bf16)
            self.start(2, m, u)

    def to_zy(self, u):
        for m in range(3):
            self.wait(2, m, u)
            self.q2[m][...] = (self.q[m][...].astype(f32) + self.r3[m][u].astype(f32)).astype(bf16)
            self.start(3, m, u)

    def last(self, u, put):
        for m in range(3):
            self.wait(3, m, u)
            put(m, (self.q2[m][...].astype(f32) + self.r4[m][u].astype(f32)).astype(bf16))


def reduce_scratch(units):
    own = [(RG, F), (RG, F), (RD, D)]
    lead = [(2,), (units, 2), (), (units,), (), (units,), (), (units,)]
    return [pltpu.VMEM(n + shape, bf16) for n in lead for shape in own] + [DMA((6, 3)), DMA((units, 6, 3))]


def put_chunk(out, m, c, value):
    if m < 2:
        for q in range(4):
            out[:, pl.ds(pl.multiple_of(q * F + c * 128, 128), 128)] = value[:, q * 128 : (q + 1) * 128]
    else:
        out[rows(c, RD), :] = value


def forward_kernel(x, sg, su, sd, h1, a0, gout, uout, wg1, wu1, wd1, wd0, acc, gb, ub, sems, wg, wu, wd, own, gsems, osem):
    at = Place()
    w = Gather(at, (wg, wu, wd), (sg, su, sd), own, gsems)
    for u in range(EARLY):
        w.fetch(u, u // C, u % C)
    greet((at.core, at.x))
    for u in range(EARLY):
        w.send(u)

    def pre(t, _):
        xt = x[pl.ds(t * T, T), :].T
        h1[:, tile(t)] = xt
        wide = xt.astype(f32)
        a0[:, tile(t)] = (wide * scale_of(wide)).astype(bf16)
        acc[:, tile(t)] = jnp.zeros((D, T), f32)
        return 0

    lax.fori_loop(0, NT, pre, 0)

    def keep(buf, out, k, i):
        return pltpu.make_async_copy(buf.at[i % 2], out.at[i // NT, :, tile(i % NT)], sems.at[k, i % 2])

    w.forward(0)

    def step(i, _):
        c, t = i // NT, i % NT

        @pl.when(t == 0)
        def _():
            w.ready(c)

        @pl.when(t == NT - 1)
        def _():
            w.forward(c + 1)

        @pl.when(i >= 2)
        def _():
            keep(gb, gout, 0, i).wait()
            keep(ub, uout, 1, i).wait()

        a = a0[:, tile(t)]
        g = dg(wg[c], a, 0, 0)
        u = dg(wu[c], a, 0, 0)
        gb[i % 2] = g
        ub[i % 2] = u
        keep(gb, gout, 0, i).start()
        keep(ub, uout, 1, i).start()
        act = (g * sigmoid(g) * u).astype(bf16)
        acc[:, tile(t)] += dg(wd[c], act, 0, 0)
        return 0

    lax.fori_loop(0, STEPS, step, 0)

    outs = [pltpu.make_async_copy(wd.at[pl.ds(0, C)], wd0, osem.at[0, 0])]
    outs[0].start()

    def post(t, _):
        h1[:, tile(t)] = (h1[:, tile(t)].astype(f32) + acc[:, tile(t)].astype(bf16).astype(f32)).astype(bf16)
        return 0

    lax.fori_loop(0, NT, post, 0)
    for u in range(C, EARLY):
        if u > C:
            w.forward(u)
        w.ready(u)
        for m, (full, out) in enumerate(((wg, wg1), (wu, wu1), (wd, wd1))):
            outs.append(pltpu.make_async_copy(full.at[u], out.at[u - C], osem.at[u - C + 1, m]))
            outs[-1].start()
    for u in range(EARLY):
        w.finish(u)
    for k in range(2):
        keep(gb, gout, 0, STEPS - 2 + k).wait()
        keep(ub, uout, 1, STEPS - 2 + k).wait()
    for out in outs:
        out.wait()


def products(g, u, da):
    s = sigmoid(g)
    sg = g * s
    da = da.astype(bf16).astype(f32)
    return (sg * u).astype(bf16), (da * u * (s + sg * (1.0 - s))).astype(bf16), (da * sg).astype(bf16)


def clear(acc, slot):
    for ref in acc:
        ref[slot] = jnp.zeros((D, F), f32)


def top_kernel(h1, dy, wg1, wu1, wd1, sg, su, sd, dh, gg, gu, gd, rawg, rawu, rawd, *scratch):
    a1, acc, dyb, accg, accu, accd, dsem, lsem, wg, wu, wd, own, gsems, *refs = scratch
    at = Place()
    grads = (accg, accu, accd)
    w = Gather(at, (wg, wu, wd), (sg, su, sd), own, gsems)
    red = Reduce(at, grads, refs)
    early = EARLY - C
    loads = [
        [pltpu.make_async_copy(src.at[u], dst.at[u], lsem.at[u, m]) for m, (src, dst) in enumerate(((wg1, wg), (wu1, wu), (wd1, wd)))]
        for u in range(early)
    ]

    def dy_copy(t):
        return pltpu.make_async_copy(dy.at[tile(t), :], dyb, dsem)

    for copy in loads[0]:
        copy.start()
    dy_copy(0).start()
    for u in range(early, C):
        w.fetch(u, 1, u)
    for load in loads[1:]:
        for copy in load:
            copy.start()
    greet((at.core, at.x, at.y, at.z))
    for u in range(early, C):
        w.send(u)

    def pre(t, _):
        wide = h1[:, tile(t)].astype(f32)
        a1[:, tile(t)] = (wide * scale_of(wide)).astype(bf16)
        acc[:, tile(t)] = jnp.zeros((D, T), f32)
        return 0

    lax.fori_loop(0, NT, pre, 0)
    for load in loads:
        for copy in load:
            copy.wait()

    outs = (gg, gu, gd)

    def step(i, _):
        c, t = i // NT, i % NT
        slot = c % 2

        @pl.when((t == 0) & (c >= 2))
        def _():
            red.to_zy(c - 2)

        @pl.when((t == 0) & (c >= 1))
        def _():
            red.to_core(c - 1, 1 - slot)

        @pl.when((t == 1) & (c >= 2))
        def _():
            red.last(c - 2, lambda m, value: put_chunk(outs[m], m, c - 2, value))

        @pl.when((t == 1) & (c >= 1))
        def _():
            red.to_x(c - 1, 1 - slot)

        @pl.when((t == 3) & (c >= 1))
        def _():
            red.to_yz(c - 1, 1 - slot)

        for u in range(early, C):

            @pl.when(i == 2 * (u - early + 1))
            def _():
                w.forward(u)

            @pl.when(i == u * NT)
            def _():
                w.ready(u)

        @pl.when(t == 0)
        def _():
            clear(grads, slot)

        @pl.when(i < NT)
        def _():
            dy_copy(i).wait()
            dh[:, tile(t)] = dyb[...].T

            @pl.when(i + 1 < NT)
            def _():
                dy_copy(i + 1).start()

        a = a1[:, tile(t)]
        y = dh[:, tile(t)]
        g = dg(wg[c], a, 0, 0)
        u = dg(wu[c], a, 0, 0)
        da = dg(wd[c], y, 1, 0)
        act, dgate, dup = products(g, u, da)
        accd[slot] += dg(y, act, 1, 1)
        accg[slot] += dg(a, dgate, 1, 1)
        accu[slot] += dg(a, dup, 1, 1)
        acc[:, tile(t)] += dg(wg[c], dgate, 1, 0) + dg(wu[c], dup, 1, 0)
        return 0

    lax.fori_loop(0, STEPS, step, 0)
    red.to_zy(C - 2)
    raw = [pltpu.make_async_copy(ref.at[(C - 1) % 2], out, lsem.at[0, m]) for m, (ref, out) in enumerate(zip(grads, (rawg, rawu, rawd)))]
    for copy in raw:
        copy.start()

    def post(t, _):
        wide = h1[:, tile(t)].astype(f32)
        scale = scale_of(wide)
        hat = wide * scale
        da = acc[:, tile(t)].astype(bf16).astype(f32)
        da = scale * (da - hat * jnp.mean(da * hat, 0, keepdims=True))
        dh[:, tile(t)] = (dh[:, tile(t)].astype(f32) + da.astype(bf16).astype(f32)).astype(bf16)
        return 0

    lax.fori_loop(0, NT, post, 0)
    red.last(C - 2, lambda m, value: put_chunk(outs[m], m, C - 2, value))
    for u in range(early, C):
        w.finish(u)
    for copy in raw:
        copy.wait()


def squares(value):
    wide = value.astype(f32)
    wide = (wide * wide).reshape(value.shape[0] // 8, 8, value.shape[1]).sum(0)
    return sum(wide[:, n * 128 : (n + 1) * 128] for n in range(value.shape[1] // 128))


def bottom_kernel(a0, dh, wd, gin, uin, rawg, rawu, rawd, gg1, gu1, gd1, gg, gu, gd, total, *scratch):
    accg, accu, accd, gb, ub, sq, everyone, sems, lsem, nsem, *refs = scratch
    at = Place()
    grads = (accg, accu, accd)
    red = Reduce(at, grads, refs)
    raw = [pltpu.make_async_copy(src, ref.at[1], lsem.at[m]) for m, (ref, src) in enumerate(zip(grads, (rawg, rawu, rawd)))]
    for copy in raw:
        copy.start()

    def load(buf, src, k, i):
        return pltpu.make_async_copy(src.at[i // NT, :, tile(i % NT)], buf.at[i % 2], sems.at[k, i % 2])

    load(gb, gin, 0, 0).start()
    load(ub, uin, 1, 0).start()
    greet((at.core, at.x, at.diag, at.y, at.z))
    outs = (gg, gu, gd)
    sq[...] = jnp.zeros((8, 128), f32)
    for out, src in zip(outs, (gg1, gu1, gd1)):
        out[1] = src[...]
    for c in range(C - 1):
        for q in range(4):
            sq[...] += squares(gg1[:, q * F + c * 128 : q * F + (c + 1) * 128]) + squares(gu1[:, q * F + c * 128 : q * F + (c + 1) * 128])
    sq[...] += squares(gd1[: (C - 1) * RD, :])

    def put(u):
        def one(m, value):
            sq[...] += squares(value)
            put_chunk(outs[m].at[jnp.where(u == 0, 1, 0)], m, jnp.where(u == 0, C - 1, u - 1), value)

        return one

    for copy in raw:
        copy.wait()

    def step(i, _):
        c, t = i // NT, i % NT
        slot = c % 2

        @pl.when((t == 0) & (c >= 2))
        def _():
            red.last(c - 2, put(c - 2))

        @pl.when((t == 0) & (c >= 1))
        def _():
            red.to_yz(c - 1, slot)

        @pl.when(t == 0)
        def _():
            red.to_core(c, 1 - slot)
            clear(grads, slot)

        @pl.when(t == 1)
        def _():
            red.to_x(c, 1 - slot)

        @pl.when((t == 2) & (c >= 1))
        def _():
            red.to_zy(c - 1)

        @pl.when(i + 1 < STEPS)
        def _():
            load(gb, gin, 0, i + 1).start()
            load(ub, uin, 1, i + 1).start()

        load(gb, gin, 0, i).wait()
        load(ub, uin, 1, i).wait()
        a = a0[:, tile(t)]
        y = dh[:, tile(t)]
        da = dg(wd[c], y, 1, 0)
        act, dgate, dup = products(gb[i % 2], ub[i % 2], da)
        accd[slot] += dg(y, act, 1, 1)
        accg[slot] += dg(a, dgate, 1, 1)
        accu[slot] += dg(a, dup, 1, 1)
        return 0

    lax.fori_loop(0, STEPS, step, 0)
    red.last(C - 2, put(C - 2))
    red.to_yz(C - 1, 0)
    red.to_core(C, 1)
    red.to_x(C, 1)
    red.to_zy(C - 1)
    red.last(C - 1, put(C - 1))
    red.to_yz(C, 1)
    red.to_zy(C)
    red.last(C, put(C))
    everyone[at.s] = sq[...]
    copies = [
        remote(sq, everyone.at[at.s], nsem.at[0, n], nsem.at[1, n], peer) for n, peer in enumerate((at.core, at.x, at.diag))
    ]
    for copy in copies:
        copy.start()
    for copy in copies:
        copy.wait()
    total[...] = everyone[0] + everyone[1] + everyone[2] + everyone[3]


def adamw_kernel(count, total, *refs):
    mean = jnp.sum(total[...], keepdims=True) / count
    factor = jnp.minimum(1.0, 0.5 * lax.rsqrt(mean + 1e-30))
    for n in range(3):
        g, w, m, v, w_out, m_out, v_out = refs[n::3]
        grad = g[...].astype(f32) * factor.reshape(1, 1, 1)
        m_new = 0.9 * m[...] + 0.1 * grad
        v_new = 0.95 * v[...] + 0.05 * grad * grad
        old = w[...].astype(f32)
        w_out[...] = (old - 0.02 * (m_new * lax.rsqrt(v_new + 1e-8) + 0.1 * old)).astype(bf16)
        m_out[...] = m_new
        v_out[...] = v_new


def params(n):
    return pltpu.CompilerParams(vmem_limit_bytes=66_500_000, collective_id=n, has_side_effects=True)


def cost(matmuls):
    return pl.CostEstimate(flops=matmuls * 2 * D * FF * TOK, bytes_accessed=1 << 26, transcendentals=0)


S = jax.ShapeDtypeStruct


def step(x, dy, *arrays):
    shards, m, v = (arrays[i : i + 3] for i in (0, 3, 6))
    early = EARLY - C
    h1, a0, g, u, wg1, wu1, wd1, wd0 = pl.pallas_call(
        forward_kernel,
        name="forward",
        in_specs=[VMEM] + [ANY] * 3,
        out_specs=[VMEM] * 2 + [ANY] * 6,
        out_shape=[S((D, TOK), bf16)] * 2
        + [S((C, F, TOK), f32)] * 2
        + [S((early, D, F), bf16)] * 2
        + [S((early, F, D), bf16), S((C, F, D), bf16)],
        scratch_shapes=[pltpu.VMEM((D, TOK), f32), pltpu.VMEM((2, F, T), f32), pltpu.VMEM((2, F, T), f32), DMA((2, 2))]
        + gather_scratch(EARLY)
        + [DMA((early + 1, 3))],
        compiler_params=params(0),
        cost_estimate=cost(3),
    )(x[0], *shards)
    dh, gg1, gu1, gd1, *raw = pl.pallas_call(
        top_kernel,
        name="top",
        in_specs=[VMEM] + [ANY] * 7,
        out_specs=[VMEM] * 4 + [ANY] * 3,
        out_shape=[S((D, TOK), bf16), S((RG, FF), bf16), S((RG, FF), bf16), S((C * RD, D), bf16)] + [S((D, F), f32)] * 3,
        scratch_shapes=[
            pltpu.VMEM((D, TOK), bf16),
            pltpu.VMEM((D, TOK), f32),
            pltpu.VMEM((T, D), bf16),
        ]
        + [pltpu.VMEM((2, D, F), f32)] * 3
        + [DMA, DMA((C, 3))]
        + gather_scratch(C)
        + reduce_scratch(C - 1),
        compiler_params=params(1),
        cost_estimate=cost(8),
    )(h1, dy[0], wg1, wu1, wd1, *shards)
    *grads, total = pl.pallas_call(
        bottom_kernel,
        name="bottom",
        in_specs=[VMEM] * 3 + [ANY] * 5 + [VMEM] * 3,
        out_specs=[VMEM] * 4,
        out_shape=[S((2, RG, FF), bf16), S((2, RG, FF), bf16), S((2, C * RD, D), bf16), S((8, 128), f32)],
        scratch_shapes=[pltpu.VMEM((2, D, F), f32)] * 3
        + [
            pltpu.VMEM((2, F, T), f32),
            pltpu.VMEM((2, F, T), f32),
            pltpu.VMEM((8, 128), f32),
            pltpu.VMEM((4, 8, 128), f32),
            DMA((2, 2)),
            DMA((3,)),
            DMA((2, 3)),
        ]
        + reduce_scratch(C + 1),
        compiler_params=params(2),
        cost_estimate=cost(4),
    )(a0, dh, wd0, g, u, *raw, gg1, gu1, gd1)
    blocks = [pl.BlockSpec((1, w.shape[1] // 2, w.shape[2]), lambda l, i: (l, i, 0)) for w in shards]
    count = 4 * sum(w.size for w in shards)
    return pl.pallas_call(
        lambda *refs: adamw_kernel(count, *refs),
        name="adamw",
        grid=(2, 2),
        in_specs=[pl.BlockSpec((8, 128), lambda l, i: (0, 0))] + blocks * 4,
        out_specs=blocks * 3,
        out_shape=[S(w.shape, bf16) for w in shards] + [S(w.shape, f32) for w in shards] * 2,
        compiler_params=pltpu.CompilerParams(vmem_limit_bytes=60_000_000),
        cost_estimate=pl.CostEstimate(flops=40 << 20, bytes_accessed=43 << 20, transcendentals=0),
    )(total, *grads, *shards, *m, *v)


def solution(mesh):
    states, cut = P(("rep", "r", "s"), None, None), P(None, "s", None)
    return jax.shard_map(
        step,
        mesh=mesh,
        in_specs=(states, states) + (cut,) * 9,
        out_specs=(P("rep", "s", None),) * 9,
        check_vma=False,
    )
```

```python
import jax
import jax.numpy as jnp
from jax import lax
from jax.experimental import pallas as pl
from jax.experimental.pallas import tpu as pltpu
from jax.sharding import PartitionSpec as P

D, FF, TOK = 640, 2048, 4096
C, F, T = 4, 512, 1024
NT = TOK // T
STEPS = C * NT
RG, RD = 160, 128
EARLY = 5
f32, bf16 = jnp.float32, jnp.bfloat16
MESH = pl.DeviceIdType.MESH
VMEM = pl.BlockSpec(memory_space=pltpu.VMEM)
ANY = pl.BlockSpec(memory_space=pl.ANY)
DMA = pltpu.SemaphoreType.DMA


def dg(a, b, ca, cb):
    return lax.dot_general(a, b, (((ca,), (cb,)), ((), ())), preferred_element_type=f32)


def sigmoid(g):
    return 0.5 * jnp.tanh(0.5 * g) + 0.5


def tile(t):
    return pl.ds(pl.multiple_of(t * T, T), T)


def rows(s, n):
    return pl.ds(pl.multiple_of(s * n, n), n)


def scale_of(wide):
    return lax.rsqrt(jnp.mean(wide * wide, 0, keepdims=True) + 1e-6)


class Place:
    def __init__(self):
        r, self.s = lax.axis_index("r"), lax.axis_index("s")
        self.chip, self.k = self.s // 2, self.s % 2
        y, z = r // 2, r % 2
        self.x_s = 2 * (1 - self.chip) + self.k
        self.core = {"s": 2 * self.chip + 1 - self.k}
        self.x = {"s": self.x_s}
        self.diag = {"s": 2 * (1 - self.chip) + 1 - self.k}
        self.y = {"r": 2 * (1 - y) + z}
        self.z = {"r": 2 * y + 1 - z}


def greet(peers):
    barrier = pltpu.get_barrier_semaphore()
    for peer in peers:
        pl.semaphore_signal(barrier, inc=1, device_id=peer, device_id_type=MESH)
    pl.semaphore_wait(barrier, len(peers))


def remote(src, dst, send, recv, peer):
    return pltpu.make_async_remote_copy(
        src_ref=src, dst_ref=dst, send_sem=send, recv_sem=recv, device_id=peer, device_id_type=MESH
    )


class Gather:
    def __init__(self, at, full, shards, own, sems):
        self.at, self.full, self.shards, self.own, self.sems = at, full, shards, own, sems

    def slot(self, m, u, s):
        return self.full[m].at[u, rows(s, RD if m else RG), :]

    def fetch(self, u, layer, c):
        for which in range(2):
            for q in range(4):
                pltpu.make_async_copy(
                    self.shards[which].at[layer, :, pl.ds(q * F + c * 128, 128)],
                    self.full[0].at[u, rows(self.at.s, RG), pl.ds(which * F + q * 128, 128)],
                    self.own.at[u, 0],
                ).start()
        pltpu.make_async_copy(self.shards[2].at[layer, pl.ds(c * RD, RD), :], self.slot(1, u, self.at.s), self.own.at[u, 1]).start()

    def copy(self, kind, m, u):
        s = self.at.x_s if kind == 2 else self.at.s
        slot = self.slot(m, u, s)
        return remote(slot, slot, self.sems.at[0, kind, u, m], self.sems.at[1, kind, u, m], self.at.x if kind == 0 else self.at.core)

    def send(self, u):
        for m in range(2):
            slot = self.slot(m, u, self.at.s)
            pltpu.make_async_copy(slot, slot, self.own.at[u, m]).wait()
            self.copy(0, m, u).start()
            self.copy(1, m, u).start()

    def forward(self, u, m):
        self.copy(0, m, u).wait_recv()
        self.copy(2, m, u).start()

    def ready(self, u, m):
        self.copy(1, m, u).wait_recv()
        self.copy(2, m, u).wait_recv()

    def finish(self, u):
        for m in range(2):
            for kind in range(3):
                self.copy(kind, m, u).wait_send()


def gather_scratch(units):
    return [
        pltpu.VMEM((units, D, 2 * F), bf16),
        pltpu.VMEM((units, F, D), bf16),
        DMA((units, 2)),
        DMA((2, 3, units, 2)),
    ]


class Reduce:
    def __init__(self, at, acc, refs):
        self.at, self.acc = at, acc
        self.p, self.r1, self.b, self.r2, self.q, self.r3, self.q2, self.r4, self.own = (refs[3 * i : 3 * i + 3] for i in range(9))
        self.ss, self.rs = refs[27:]

    def term(self, m, slot, s):
        if m < 2:
            return self.acc[0][slot, rows(s, RG), m * F : (m + 1) * F]
        return self.acc[1][slot, :, rows(s, RD)].T

    def half(self, m, n):
        h = (RG if m < 2 else RD) // 2
        return pl.ds(n * h, h)

    def copies(self, stage, m, u):
        at, v = self.at, u % 2
        if stage == 0:
            return [remote(self.p[m], self.r1[m].at[v], self.ss.at[0, m], self.rs.at[v, 0, m], at.core)]
        if stage == 1:
            return [remote(self.b[m], self.r2[m].at[v], self.ss.at[1, m], self.rs.at[v, 1, m], at.x)]
        src, dst, ways = (self.q, self.r3, (at.y, at.z)) if stage == 2 else (self.q2, self.r4, (at.z, at.y))
        return [
            remote(src[m].at[self.half(m, n)], dst[m].at[v, self.half(m, n)], self.ss.at[2 * stage - 2 + n, m], self.rs.at[v, 2 * stage - 2 + n, m], ways[n])
            for n in range(2)
        ]

    def start(self, stage, m, u):
        for copy in self.copies(stage, m, u):
            copy.start()

    def wait(self, stage, m, u):
        for copy in self.copies(stage, m, u):
            copy.wait()

    def to_core(self, u, slot, which=range(3)):
        for m in which:
            for j in range(2):
                self.p[m][j] = self.term(m, slot, 2 * j + 1 - self.at.k).astype(bf16)
            self.start(0, m, u)

    def to_x(self, u, slot, which=range(3)):
        at = self.at
        for m in which:
            self.wait(0, m, u)
            self.b[m][...] = (self.term(m, slot, at.x_s) + self.r1[m][u % 2, 1 - at.chip].astype(f32)).astype(bf16)
            self.start(1, m, u)
        for m in which:
            self.own[m][...] = self.term(m, slot, at.s) + self.r1[m][u % 2, at.chip].astype(f32)

    def to_yz(self, u, which=range(3)):
        for m in which:
            self.wait(1, m, u)
            self.q[m][...] = (self.own[m][...] + self.r2[m][u % 2].astype(f32)).astype(bf16)
            self.start(2, m, u)

    def to_zy(self, u, which=range(3)):
        for m in which:
            self.wait(2, m, u)
            self.q2[m][...] = (self.q[m][...].astype(f32) + self.r3[m][u % 2].astype(f32)).astype(bf16)
            self.start(3, m, u)

    def last(self, u, put, which=range(3)):
        for m in which:
            self.wait(3, m, u)
            put(m, (self.q2[m][...].astype(f32) + self.r4[m][u % 2].astype(f32)).astype(bf16))


def reduce_scratch():
    own = [(RG, F), (RG, F), (RD, D)]
    lead = [(2,), (2, 2), (), (2,), (), (2,), (), (2,)]
    buffers = [pltpu.VMEM(n + shape, bf16) for n in lead for shape in own]
    return buffers + [pltpu.VMEM(shape, f32) for shape in own] + [DMA((6, 3)), DMA((2, 6, 3))]


def put_chunk(out, m, c, value):
    if m < 2:
        for q in range(4):
            out[:, pl.ds(pl.multiple_of(q * F + c * 128, 128), 128)] = value[:, q * 128 : (q + 1) * 128]
    else:
        out[rows(c, RD), :] = value


def forward_kernel(x, dy, sg, su, sd, h1_out, a0_out, dyt_out, gout, uout, wgu1, wd1, wd0, h1, a0, acc, xb, yb, gb, ub, sems, wgu, wd, own, gsems, osem, xsem, ysem):
    at = Place()
    w = Gather(at, (wgu, wd), (sg, su, sd), own, gsems)
    w.fetch(0, 0, 0)
    xs = [pltpu.make_async_copy(x.at[pl.ds(t * T, T), :], xb.at[pl.ds(t * T, T), :], xsem.at[t]) for t in range(NT)]
    xs[0].start()
    greet((at.core, at.x))
    w.send(0)
    for u in range(1, EARLY):
        w.fetch(u, u // C, u % C)
        if u < NT:
            xs[u].start()
    for u in range(1, EARLY):
        w.send(u)

    outs = []
    ys = [pltpu.make_async_copy(dy.at[pl.ds(t * T, T), :], xb.at[pl.ds(t * T, T), :], xsem.at[t]) for t in range(NT)]
    for t in range(NT):
        here = slice(t * T, (t + 1) * T)
        xs[t].wait()
        xt = xb[here, :].T
        h1[:, here] = xt
        wide = xt.astype(f32)
        a0[:, here] = (wide * scale_of(wide)).astype(bf16)
        ys[t].start()
        acc[:, here] = jnp.zeros((D, T), f32)
        outs.append(pltpu.make_async_copy(a0.at[:, pl.ds(t * T, T)], a0_out.at[:, pl.ds(t * T, T)], ysem.at[0, t]))
        outs[-1].start()
    for t in range(NT):
        ys[t].wait()
        yb[:, t * T : (t + 1) * T] = xb[t * T : (t + 1) * T, :].T
        outs.append(pltpu.make_async_copy(yb.at[:, pl.ds(t * T, T)], dyt_out.at[:, pl.ds(t * T, T)], ysem.at[1, t]))
        outs[-1].start()

    def keep(buf, out, k, i):
        return pltpu.make_async_copy(buf.at[i % 2], out.at[i // NT, :, tile(i % NT)], sems.at[k, i % 2])

    for m in range(2):
        w.forward(0, m)
        w.ready(0, m)

    def step(i, _):
        c, t = i // NT, i % NT

        @pl.when((t == 0) & (c >= 1))
        def _():
            w.ready(c, 0)
            w.ready(c, 1)

        @pl.when(t == NT - 1)
        def _():
            w.forward(c + 1, 0)
            w.forward(c + 1, 1)

        @pl.when(i >= 2)
        def _():
            keep(gb, gout, 0, i).wait()
            keep(ub, uout, 1, i).wait()

        both = dg(wgu[c], a0[:, tile(t)], 0, 0)
        g, u = both[:F], both[F:]
        gb[i % 2] = g
        ub[i % 2] = u
        keep(gb, gout, 0, i).start()
        keep(ub, uout, 1, i).start()
        act = (g * sigmoid(g) * u).astype(bf16)

        acc[:, tile(t)] += dg(wd[c], act, 0, 0)
        return 0

    lax.fori_loop(0, STEPS, step, 0)


    outs.append(pltpu.make_async_copy(wd.at[pl.ds(0, C)], wd0, osem.at[0, 0]))
    outs[-1].start()
    for t in range(NT):
        here = slice(t * T, (t + 1) * T)
        h1[:, here] = (h1[:, here].astype(f32) + acc[:, here].astype(bf16).astype(f32)).astype(bf16)
        outs.append(pltpu.make_async_copy(h1.at[:, pl.ds(t * T, T)], h1_out.at[:, pl.ds(t * T, T)], ysem.at[2, t]))
        outs[-1].start()
    for u in range(C, EARLY):
        for m, (full, out) in enumerate(((wgu, wgu1), (wd, wd1))):
            if u > C:
                w.forward(u, m)
            w.ready(u, m)
            outs.append(pltpu.make_async_copy(full.at[u], out.at[u - C], osem.at[u - C + 1, m]))
            outs[-1].start()
    for u in range(EARLY):
        w.finish(u)
    for k in range(2):
        keep(gb, gout, 0, STEPS - 2 + k).wait()
        keep(ub, uout, 1, STEPS - 2 + k).wait()
    for out in outs:
        out.wait()


def products(g, u, da):
    s = sigmoid(g)
    sg = g * s
    da = da.astype(bf16).astype(f32)
    return (sg * u).astype(bf16), (da * u * (s + sg * (1.0 - s))).astype(bf16), (da * sg).astype(bf16)


def clear(acc, slot):
    for ref in acc:
        ref[slot] = jnp.zeros(ref.shape[1:], f32)


def top_kernel(h1_in, dyt, wgu1, wd1, sg, su, sd, dh_out, gg, gu, gd, rawgu, rawd, *scratch):
    h1, dh, a1, acc, scales, dgu, accgu, accd, tsem, lsem, wgu, wd, own, gsems, *refs = scratch
    at = Place()
    grads = (accgu, accd)
    w = Gather(at, (wgu, wd), (sg, su, sd), own, gsems)
    red = Reduce(at, grads, refs)
    early = EARLY - C
    loads = [
        [pltpu.make_async_copy(src.at[u], dst.at[u], lsem.at[u, m]) for m, (src, dst) in enumerate(((wgu1, wgu), (wd1, wd)))]
        for u in range(early)
    ]

    def columns(src, dst, k, t):
        return pltpu.make_async_copy(src.at[:, tile(t)], dst.at[:, tile(t)], tsem.at[k, t])

    columns(h1_in, h1, 0, 0).start()
    for copy in loads[0]:
        copy.start()
    for u in range(early, C):
        w.fetch(u, 1, u)
    for t in range(1, NT):
        columns(h1_in, h1, 0, t).start()
    for t in range(NT):
        columns(dyt, dh, 1, t).start()
    for load in loads[1:]:
        for copy in load:
            copy.start()
    greet((at.core, at.x, at.y, at.z))
    for u in range(early, C):
        w.send(u)

    def pre(t, _):
        columns(h1_in, h1, 0, t).wait()
        wide = h1[:, tile(t)].astype(f32)
        scale = scale_of(wide)
        scales[:, tile(t)] = scale
        a1[:, tile(t)] = (wide * scale).astype(bf16)
        acc[:, tile(t)] = jnp.zeros((D, T), f32)
        return 0

    lax.fori_loop(0, NT, pre, 0)
    for load in loads:
        for copy in load:
            copy.wait()
    for t in range(NT):
        columns(dyt, dh, 1, t).wait()

    outs = (gg, gu, gd)

    def step(i, _):
        c, t = i // NT, i % NT
        slot = c % 2

        @pl.when((t == 0) & (c >= 2))
        def _():
            red.to_zy(c - 2)

        @pl.when((t == 0) & (c >= 1))
        def _():
            red.to_core(c - 1, 1 - slot)

        @pl.when((t == 1) & (c >= 2))
        def _():
            red.last(c - 2, lambda m, value: put_chunk(outs[m], m, c - 2, value))

        @pl.when((t == 1) & (c >= 1))
        def _():
            red.to_x(c - 1, 1 - slot)

        @pl.when((t == 3) & (c >= 1))
        def _():
            red.to_yz(c - 1)

        for u in range(early, C):

            @pl.when(i == 2 * (u - early) + 2)
            def _():
                w.forward(u, 0)
                w.forward(u, 1)

            @pl.when(i == u * NT)
            def _():
                w.ready(u, 0)
                w.ready(u, 1)

        @pl.when(t == 0)
        def _():
            clear(grads, slot)

        a = a1[:, tile(t)]
        y = dh[:, tile(t)]
        both = dg(wgu[c], a, 0, 0)
        act, dgu[:F], dgu[F:] = products(both[:F], both[F:], dg(wd[c], y, 1, 0))
        accd[slot] += dg(y, act, 1, 1)
        accgu[slot] += dg(a, dgu[...], 1, 1)
        acc[:, tile(t)] += dg(wgu[c], dgu[...], 1, 0)
        return 0

    lax.fori_loop(0, STEPS, step, 0)
    red.to_zy(C - 2)
    raw = [pltpu.make_async_copy(ref.at[(C - 1) % 2], out, lsem.at[0, m]) for m, (ref, out) in enumerate(zip(grads, (rawgu, rawd)))]
    for copy in raw:
        copy.start()


    def post(t, _):
        scale = scales[:, tile(t)]
        wide = h1[:, tile(t)].astype(f32)
        da = acc[:, tile(t)].astype(bf16).astype(f32)
        along = scale * scale * scale * jnp.mean(da * wide, 0, keepdims=True)
        dh[:, tile(t)] = (dh[:, tile(t)].astype(f32) + (scale * da - along * wide).astype(bf16).astype(f32)).astype(bf16)
        columns(dh, dh_out, 0, t).start()
        return 0

    lax.fori_loop(0, NT, post, 0)
    red.last(C - 2, lambda m, value: put_chunk(outs[m], m, C - 2, value))
    for u in range(early, C):
        w.finish(u)
    for copy in raw:
        copy.wait()
    for t in range(NT):
        columns(dh, dh_out, 0, t).wait()


def squares(value):
    wide = value.astype(f32)
    wide = (wide * wide).reshape(value.shape[0] // 8, 8, value.shape[1]).sum(0)
    return sum(wide[:, n * 128 : (n + 1) * 128] for n in range(value.shape[1] // 128))


def bottom_kernel(a0_in, dh_in, wd_in, gin, uin, rawgu, rawd, gg1, gu1, gd1, gg_out, gu_out, gd_out, total, *scratch):
    a0, dh, wd, gg, gu, gd, accgu, accd, gb, ub, sq, everyone, sems, lsem, nsem, tsem, fsem, *refs = scratch
    at = Place()
    grads = (accgu, accd)
    red = Reduce(at, grads, refs)
    raw = [pltpu.make_async_copy(src, ref.at[1], lsem.at[m]) for m, (ref, src) in enumerate(zip(grads, (rawgu, rawd)))]

    def load(buf, src, k, i):
        return pltpu.make_async_copy(src.at[i // NT, :, tile(i % NT)], buf.at[i % 2], sems.at[k, i % 2])

    def tiles(t):
        return [
            pltpu.make_async_copy(dh_in.at[:, tile(t)], dh.at[:, tile(t)], tsem.at[0, t]),
            pltpu.make_async_copy(a0_in.at[:, tile(t)], a0.at[:, tile(t)], tsem.at[1, t]),
            pltpu.make_async_copy(wd_in.at[t], wd.at[t], tsem.at[2, t]),
        ]

    outs = (gg, gu, gd)
    done = [pltpu.make_async_copy(src, ref.at[1], fsem.at[0, m]) for m, (ref, src) in enumerate(zip(outs, (gg1, gu1, gd1)))]
    for copy in tiles(0):
        copy.start()
    load(gb, gin, 0, 0).start()
    load(ub, uin, 1, 0).start()
    for copy in tiles(1) + raw + tiles(2) + tiles(3) + done:
        copy.start()
    greet((at.core, at.x, at.diag, at.y, at.z))
    sq[...] = jnp.zeros((8, 128), f32)

    def put(u):
        def one(m, value):
            sq[...] += squares(value)
            put_chunk(outs[m].at[jnp.where(u == 0, 1, 0)], m, jnp.where(u == 0, C - 1, u - 1), value)

        return one

    def step(i, _):
        c, t = i // NT, i % NT
        slot = c % 2

        @pl.when(i < NT)
        def _():
            for copy in tiles(t):
                copy.wait()

        @pl.when(i == 1)
        def _():
            for copy in raw + done:
                copy.wait()

            red.to_core(0, 1)

        @pl.when((t == 0) & (c >= 1))
        def _():
            red.to_core(c, 1 - slot)

        @pl.when(t == 0)
        def _():
            clear(grads, slot)

        @pl.when((t == 1) & (c >= 2))
        def _():
            red.last(c - 2, put(c - 2))

        @pl.when((t == 1) & (c >= 1))
        def _():
            red.to_yz(c - 1)

        @pl.when(((t == 1) & (c >= 1)) | (i == 2))
        def _():
            red.to_x(c, 1 - slot)

        @pl.when((t == 3) & (c >= 1))
        def _():
            red.to_zy(c - 1)

        @pl.when(i + 1 < STEPS)
        def _():
            load(gb, gin, 0, i + 1).start()
            load(ub, uin, 1, i + 1).start()

        load(gb, gin, 0, i).wait()
        load(ub, uin, 1, i).wait()
        a = a0[:, tile(t)]
        y = dh[:, tile(t)]
        da = dg(wd[c], y, 1, 0)
        act, dgate, dup = products(gb[i % 2], ub[i % 2], da)
        accd[slot] += dg(y, act, 1, 1)
        accgu[slot] += dg(a, jnp.concatenate([dgate, dup], 0), 1, 1)
        return 0

    lax.fori_loop(0, STEPS, step, 0)
    red.to_core(C, 1)
    red.last(C - 2, put(C - 2))
    red.to_yz(C - 1)
    red.to_x(C, 1)
    red.to_zy(C - 1)
    for c in range(C - 1):
        for q in range(4):
            sq[...] += squares(gg[1, :, q * F + c * 128 : q * F + (c + 1) * 128]) + squares(gu[1, :, q * F + c * 128 : q * F + (c + 1) * 128])
    sq[...] += squares(gd[1, : (C - 1) * RD, :])
    late = [
        [pltpu.make_async_copy(ref.at[l], out.at[l], fsem.at[1 + l, m]) for m, (ref, out) in enumerate(zip(outs, (gg_out, gu_out, gd_out)))]
        for l in range(2)
    ]
    for copy in late[1]:
        copy.start()
    red.to_yz(C, (0,))
    red.to_yz(C, (1,))
    red.last(C - 1, put(C - 1))
    red.to_zy(C, (0,))
    red.to_yz(C, (2,))
    red.to_zy(C, (1,))
    red.last(C, put(C), (0,))
    red.to_zy(C, (2,))
    red.last(C, put(C), (1,))
    red.last(C, put(C), (2,))
    for copy in late[0]:
        copy.start()
    everyone[at.s] = sq[...]
    copies = [
        remote(sq, everyone.at[at.s], nsem.at[0, n], nsem.at[1, n], peer) for n, peer in enumerate((at.core, at.x, at.diag))
    ]
    for copy in copies:
        copy.start()
    for copy in copies:
        copy.wait()
    total[...] = everyone[0] + everyone[1] + everyone[2] + everyone[3]
    for copy in late[0] + late[1]:
        copy.wait()


def adamw_kernel(count, total, *refs):
    mean = jnp.sum(total[...], keepdims=True) / count
    factor = jnp.minimum(1.0, 0.5 * lax.rsqrt(mean + 1e-30))
    for n in range(3):
        g, w, m, v, w_out, m_out, v_out = refs[n::3]
        grad = g[...].astype(f32) * factor.reshape(1, 1, 1)
        m_new = 0.9 * m[...] + 0.1 * grad
        v_new = 0.95 * v[...] + 0.05 * grad * grad
        old = w[...].astype(f32)
        w_out[...] = (old - 0.02 * (m_new * lax.rsqrt(v_new + 1e-8) + 0.1 * old)).astype(bf16)
        m_out[...] = m_new
        v_out[...] = v_new


def params(n):
    return pltpu.CompilerParams(vmem_limit_bytes=67_000_000, collective_id=n, has_side_effects=True)


def cost(matmuls):
    return pl.CostEstimate(flops=matmuls * 2 * D * FF * TOK, bytes_accessed=1 << 26, transcendentals=0)


S = jax.ShapeDtypeStruct


def step(x, dy, *arrays):
    shards, m, v = (arrays[i : i + 3] for i in (0, 3, 6))
    early = EARLY - C
    h1, a0, dyt, g, u, wgu1, wd1, wd0 = pl.pallas_call(
        forward_kernel,
        name="forward",
        in_specs=[ANY] * 5,
        out_specs=[ANY] * 8,
        out_shape=[S((D, TOK), bf16)] * 3
        + [S((C, F, TOK), f32)] * 2
        + [S((early, D, 2 * F), bf16), S((early, F, D), bf16), S((C, F, D), bf16)],
        scratch_shapes=[pltpu.VMEM((D, TOK), bf16)] * 2
        + [pltpu.VMEM((D, TOK), f32), pltpu.VMEM((TOK, D), bf16), pltpu.VMEM((D, TOK), bf16), pltpu.VMEM((2, F, T), f32), pltpu.VMEM((2, F, T), f32), DMA((2, 2))]
        + gather_scratch(EARLY)
        + [DMA((early + 1, 2)), DMA((NT,)), DMA((3, NT))],
        compiler_params=params(0),
        cost_estimate=cost(3),
    )(x[0], dy[0], *shards)
    dh, gg1, gu1, gd1, *raw = pl.pallas_call(
        top_kernel,
        name="top",
        in_specs=[ANY] * 7,
        out_specs=[ANY] + [VMEM] * 3 + [ANY] * 2,
        out_shape=[S((D, TOK), bf16), S((RG, FF), bf16), S((RG, FF), bf16), S((C * RD, D), bf16)] + [S((D, 2 * F), f32), S((D, F), f32)],
        scratch_shapes=[
            pltpu.VMEM((D, TOK), bf16),
            pltpu.VMEM((D, TOK), bf16),
            pltpu.VMEM((D, TOK), bf16),
            pltpu.VMEM((D, TOK), f32),
            pltpu.VMEM((1, TOK), f32),
            pltpu.VMEM((2 * F, T), bf16),
            pltpu.VMEM((2, D, 2 * F), f32),
            pltpu.VMEM((2, D, F), f32),
        ]
        + [DMA((2, NT)), DMA((C, 2))]
        + gather_scratch(C)
        + reduce_scratch(),
        compiler_params=params(1),
        cost_estimate=cost(8),
    )(h1, dyt, wgu1, wd1, *shards)
    *grads, total = pl.pallas_call(
        bottom_kernel,
        name="bottom",
        in_specs=[ANY] * 10,
        out_specs=[ANY] * 3 + [VMEM],
        out_shape=[S((2, RG, FF), bf16), S((2, RG, FF), bf16), S((2, C * RD, D), bf16), S((8, 128), f32)],
        scratch_shapes=[
            pltpu.VMEM((D, TOK), bf16),
            pltpu.VMEM((D, TOK), bf16),
            pltpu.VMEM((C, F, D), bf16),
            pltpu.VMEM((2, RG, FF), bf16),
            pltpu.VMEM((2, RG, FF), bf16),
            pltpu.VMEM((2, C * RD, D), bf16),
            pltpu.VMEM((2, D, 2 * F), f32),
            pltpu.VMEM((2, D, F), f32),
            pltpu.VMEM((2, F, T), f32),
            pltpu.VMEM((2, F, T), f32),
            pltpu.VMEM((8, 128), f32),
            pltpu.VMEM((4, 8, 128), f32),
            DMA((2, 2)),
            DMA((2,)),
            DMA((2, 3)),
            DMA((3, NT)),
            DMA((3, 3)),
        ]
        + reduce_scratch(),
        compiler_params=params(2),
        cost_estimate=cost(4),
    )(a0, dh, wd0, g, u, *raw, gg1, gu1, gd1)
    blocks = [pl.BlockSpec((1, w.shape[1] // 2, w.shape[2]), lambda l, i: (l, i, 0)) for w in shards]
    count = 4 * sum(w.size for w in shards)
    return pl.pallas_call(
        lambda *refs: adamw_kernel(count, *refs),
        name="adamw",
        grid=(2, 2),
        in_specs=[pl.BlockSpec((8, 128), lambda l, i: (0, 0))] + blocks * 4,
        out_specs=blocks * 3,
        out_shape=[S(w.shape, bf16) for w in shards] + [S(w.shape, f32) for w in shards] * 2,
        compiler_params=pltpu.CompilerParams(vmem_limit_bytes=60_000_000),
        cost_estimate=pl.CostEstimate(flops=40 << 20, bytes_accessed=43 << 20, transcendentals=0),
    )(total, *grads, *shards, *m, *v)


def solution(mesh):
    states, cut = P(("rep", "r", "s"), None, None), P(None, "s", None)
    return jax.shard_map(
        step,
        mesh=mesh,
        in_specs=(states, states) + (cut,) * 9,
        out_specs=(P("rep", "s", None),) * 9,
        check_vma=False,
    )
```

```python
import jax
import jax.numpy as jnp
from jax import lax
from jax.experimental import pallas as pl
from jax.experimental.pallas import tpu as pltpu
from jax.sharding import PartitionSpec as P

D, FF, TOK = 640, 2048, 4096
C, F, T = 4, 512, 1024
NT = TOK // T
STEPS = C * NT
RG, RD = 160, 128
EARLY = 5
f32, bf16 = jnp.float32, jnp.bfloat16
MESH = pl.DeviceIdType.MESH
VMEM = pl.BlockSpec(memory_space=pltpu.VMEM)
ANY = pl.BlockSpec(memory_space=pl.ANY)
DMA = pltpu.SemaphoreType.DMA


def dg(a, b, ca, cb):
    return lax.dot_general(a, b, (((ca,), (cb,)), ((), ())), preferred_element_type=f32)


def sigmoid(g):
    return 0.5 * jnp.tanh(0.5 * g) + 0.5


def tile(t):
    return pl.ds(pl.multiple_of(t * T, T), T)


def rows(s, n):
    return pl.ds(pl.multiple_of(s * n, n), n)


def scale_of(wide):
    return lax.rsqrt(jnp.mean(wide * wide, 0, keepdims=True) + 1e-6)


class Place:
    def __init__(self):
        r, self.s = lax.axis_index("r"), lax.axis_index("s")
        self.chip, self.k = self.s // 2, self.s % 2
        y, z = r // 2, r % 2
        self.y_at = y
        self.x_s = 2 * (1 - self.chip) + self.k
        self.core = {"s": 2 * self.chip + 1 - self.k}
        self.x = {"s": self.x_s}
        self.diag = {"s": 2 * (1 - self.chip) + 1 - self.k}
        self.y = {"r": 2 * (1 - y) + z}
        self.z = {"r": 2 * y + 1 - z}


def greet(peers):
    barrier = pltpu.get_barrier_semaphore()
    for peer in peers:
        pl.semaphore_signal(barrier, inc=1, device_id=peer, device_id_type=MESH)
    pl.semaphore_wait(barrier, len(peers))


def remote(src, dst, send, recv, peer):
    return pltpu.make_async_remote_copy(
        src_ref=src, dst_ref=dst, send_sem=send, recv_sem=recv, device_id=peer, device_id_type=MESH
    )


class Gather:
    def __init__(self, at, full, shards, own, sems, shared):
        self.at, self.full, self.shards, self.own, self.sems, self.shared = at, full, shards, own, sems, shared

    def slot(self, m, u, s):
        return self.full[m].at[u, rows(s, RD if m else RG), :]

    def fetch(self, u, layer, c):
        for which in range(2):
            for q in range(4):
                pltpu.make_async_copy(
                    self.shards[which].at[layer, :, pl.ds(q * F + c * 128, 128)],
                    self.full[0].at[u, rows(self.at.s, RG), pl.ds(which * F + q * 128, 128)],
                    self.own.at[u, 0],
                ).start()
        pltpu.make_async_copy(self.shards[2].at[layer, pl.ds(c * RD, RD), :], self.slot(1, u, self.at.s), self.own.at[u, 1]).start()

    def split(self, m, u):
        return self.shared and m == 1 and not (isinstance(u, int) and u == 0)

    def copy(self, kind, m, u):
        at = self.at
        s = at.x_s if kind >= 2 else at.s
        slot = self.slot(m, u, s)
        if self.split(m, u) and kind != 1:
            h = RD // 2
            slot = self.full[m].at[u, pl.ds(pl.multiple_of(s * RD + (1 - at.y_at if kind == 4 else at.y_at) * h, h), h), :]
        peer = (at.x, at.core, at.core, at.y, at.core)[kind]
        return remote(slot, slot, self.sems.at[0, kind, u, m], self.sems.at[1, kind, u, m], peer)

    def send(self, u):
        for m in (1, 0) if self.split(1, u) else (0, 1):
            slot = self.slot(m, u, self.at.s)
            pltpu.make_async_copy(slot, slot, self.own.at[u, m]).wait()
            self.copy(0, m, u).start()
            self.copy(1, m, u).start()

    def forward(self, u, m):
        self.copy(0, m, u).wait_recv()
        self.copy(2, m, u).start()
        if self.split(m, u):
            self.copy(3, m, u).start()

    def forward_other(self, u):
        self.copy(3, 1, u).wait_recv()
        self.copy(4, 1, u).start()

    def ready(self, u, m):
        self.copy(1, m, u).wait_recv()
        self.copy(2, m, u).wait_recv()
        if self.split(m, u):
            self.copy(4, m, u).wait_recv()

    def finish(self, u):
        for m in range(2):
            for kind in range(5 if self.split(m, u) else 3):
                self.copy(kind, m, u).wait_send()


def gather_scratch(units):
    return [
        pltpu.VMEM((units, D, 2 * F), bf16),
        pltpu.VMEM((units, F, D), bf16),
        DMA((units, 2)),
        DMA((2, 5, units, 2)),
    ]


class Reduce:
    def __init__(self, at, acc, refs):
        self.at, self.acc = at, acc
        self.p, self.r1, self.b, self.r2, self.q, self.r3, self.q2, self.r4, self.own = (refs[3 * i : 3 * i + 3] for i in range(9))
        self.ss, self.rs = refs[27:]

    def term(self, m, slot, s):
        if m < 2:
            return self.acc[0][slot, rows(s, RG), m * F : (m + 1) * F]
        return self.acc[1][slot, :, rows(s, RD)].T

    def half(self, m, n):
        h = (RG if m < 2 else RD) // 2
        return pl.ds(n * h, h)

    def copies(self, stage, m, u):
        at, v = self.at, u % 2
        if stage == 0:
            return [remote(self.p[m], self.r1[m].at[v], self.ss.at[0, m], self.rs.at[v, 0, m], at.core)]
        if stage == 1:
            return [remote(self.b[m], self.r2[m].at[v], self.ss.at[1, m], self.rs.at[v, 1, m], at.x)]
        src, dst, ways = (self.q, self.r3, (at.y, at.z)) if stage == 2 else (self.q2, self.r4, (at.z, at.y))
        return [
            remote(src[m].at[self.half(m, n)], dst[m].at[v, self.half(m, n)], self.ss.at[2 * stage - 2 + n, m], self.rs.at[v, 2 * stage - 2 + n, m], ways[n])
            for n in range(2)
        ]

    def start(self, stage, m, u):
        for copy in self.copies(stage, m, u):
            copy.start()

    def wait(self, stage, m, u):
        for copy in self.copies(stage, m, u):
            copy.wait()

    def to_core(self, u, slot, which=range(3)):
        for m in which:
            for j in range(2):
                self.p[m][j] = self.term(m, slot, 2 * j + 1 - self.at.k).astype(bf16)
            self.start(0, m, u)

    def to_x(self, u, slot, which=range(3)):
        at = self.at
        for m in which:
            self.wait(0, m, u)
            self.b[m][...] = (self.term(m, slot, at.x_s) + self.r1[m][u % 2, 1 - at.chip].astype(f32)).astype(bf16)
            self.start(1, m, u)
        for m in which:
            self.own[m][...] = self.term(m, slot, at.s) + self.r1[m][u % 2, at.chip].astype(f32)

    def to_yz(self, u, which=range(3)):
        for m in which:
            self.wait(1, m, u)
            self.q[m][...] = (self.own[m][...] + self.r2[m][u % 2].astype(f32)).astype(bf16)
            self.start(2, m, u)

    def to_zy(self, u, which=range(3)):
        for m in which:
            self.wait(2, m, u)
            self.q2[m][...] = (self.q[m][...].astype(f32) + self.r3[m][u % 2].astype(f32)).astype(bf16)
            self.start(3, m, u)

    def last(self, u, put, which=range(3)):
        for m in which:
            self.wait(3, m, u)
            put(m, (self.q2[m][...].astype(f32) + self.r4[m][u % 2].astype(f32)).astype(bf16))


def reduce_scratch():
    own = [(RG, F), (RG, F), (RD, D)]
    lead = [(2,), (2, 2), (), (2,), (), (2,), (), (2,)]
    buffers = [pltpu.VMEM(n + shape, bf16) for n in lead for shape in own]
    return buffers + [pltpu.VMEM(shape, f32) for shape in own] + [DMA((6, 3)), DMA((2, 6, 3))]


def put_chunk(out, m, c, value):
    if m < 2:
        for q in range(4):
            out[:, pl.ds(pl.multiple_of(q * F + c * 128, 128), 128)] = value[:, q * 128 : (q + 1) * 128]
    else:
        out[rows(c, RD), :] = value


def forward_kernel(x, dy, sg, su, sd, h1_out, a0_out, dyt_out, gout, uout, wgu1, wd1, wd0, h1, a0, acc, xb, yb, gb, ub, acts, sems, wgu, wd, own, gsems, osem, xsem, ysem):
    at = Place()
    w = Gather(at, (wgu, wd), (sg, su, sd), own, gsems, True)
    w.fetch(0, 0, 0)
    xs = [pltpu.make_async_copy(x.at[pl.ds(t * T, T), :], xb.at[pl.ds(t * T, T), :], xsem.at[t]) for t in range(NT)]
    xs[0].start()
    greet((at.core, at.x, at.y))
    w.send(0)
    for u in range(1, EARLY):
        w.fetch(u, u // C, u % C)
        if u < NT:
            xs[u].start()
    for u in range(1, EARLY):
        w.send(u)

    outs = []
    ys = [pltpu.make_async_copy(dy.at[pl.ds(t * T, T), :], xb.at[pl.ds(t * T, T), :], xsem.at[t]) for t in range(NT)]
    for t in range(NT):
        here = slice(t * T, (t + 1) * T)
        xs[t].wait()
        xt = xb[here, :].T
        h1[:, here] = xt
        wide = xt.astype(f32)
        a0[:, here] = (wide * scale_of(wide)).astype(bf16)
        ys[t].start()
        acc[:, here] = jnp.zeros((D, T), f32)
        outs.append(pltpu.make_async_copy(a0.at[:, pl.ds(t * T, T)], a0_out.at[:, pl.ds(t * T, T)], ysem.at[0, t]))
        outs[-1].start()
    for t in range(NT):
        ys[t].wait()
        yb[:, t * T : (t + 1) * T] = xb[t * T : (t + 1) * T, :].T
        outs.append(pltpu.make_async_copy(yb.at[:, pl.ds(t * T, T)], dyt_out.at[:, pl.ds(t * T, T)], ysem.at[1, t]))
        outs[-1].start()

    def keep(buf, out, k, i):
        return pltpu.make_async_copy(buf.at[i % 2], out.at[i // NT, :, tile(i % NT)], sems.at[k, i % 2])

    def activation(i, c, t):
        both = dg(wgu[c], a0[:, tile(t)], 0, 0)
        g, u = both[:F], both[F:]
        gb[i % 2] = g
        ub[i % 2] = u
        keep(gb, gout, 0, i).start()
        keep(ub, uout, 1, i).start()
        return (g * sigmoid(g) * u).astype(bf16)

    w.forward(0, 0)
    w.ready(0, 0)

    def first(t, _):
        acts[t] = activation(t, 0, t)
        return 0

    lax.fori_loop(0, 2, first, 0)
    w.forward(0, 1)
    w.ready(0, 1)

    def second(t, _):
        acc[:, tile(t)] = dg(wd[0], acts[t], 0, 0)
        return 0

    lax.fori_loop(0, 2, second, 0)
    w.forward(jnp.int32(1), 1)

    def step(i, _):
        c, t = i // NT, i % NT

        @pl.when((t == 0) & (c >= 1))
        def _():
            w.ready(c, 0)
            w.ready(c, 1)

        @pl.when(t == 1)
        def _():
            w.forward(c + 1, 1)

        @pl.when(t == NT - 1)
        def _():
            w.forward_other(c + 1)
            w.forward(c + 1, 0)

        keep(gb, gout, 0, i).wait()
        keep(ub, uout, 1, i).wait()
        acc[:, tile(t)] += dg(wd[c], activation(i, c, t), 0, 0)
        return 0

    lax.fori_loop(2, STEPS, step, 0)


    outs.append(pltpu.make_async_copy(wd.at[pl.ds(0, C)], wd0, osem.at[0, 0]))
    outs[-1].start()
    for t in range(NT):
        here = slice(t * T, (t + 1) * T)
        h1[:, here] = (h1[:, here].astype(f32) + acc[:, here].astype(bf16).astype(f32)).astype(bf16)
        outs.append(pltpu.make_async_copy(h1.at[:, pl.ds(t * T, T)], h1_out.at[:, pl.ds(t * T, T)], ysem.at[2, t]))
        outs[-1].start()
    for u in range(C, EARLY):
        for m, (full, out) in enumerate(((wgu, wgu1), (wd, wd1))):
            if u > C:
                w.forward(u, m)
            w.ready(u, m)
            outs.append(pltpu.make_async_copy(full.at[u], out.at[u - C], osem.at[u - C + 1, m]))
            outs[-1].start()
    for u in range(EARLY):
        w.finish(u)
    for k in range(2):
        keep(gb, gout, 0, STEPS - 2 + k).wait()
        keep(ub, uout, 1, STEPS - 2 + k).wait()
    for out in outs:
        out.wait()


def products(g, u, da):
    s = sigmoid(g)
    sg = g * s
    da = da.astype(bf16).astype(f32)
    return (sg * u).astype(bf16), (da * u * (s + sg * (1.0 - s))).astype(bf16), (da * sg).astype(bf16)


def clear(acc, slot):
    for ref in acc:
        ref[slot] = jnp.zeros(ref.shape[1:], f32)


def top_kernel(h1_in, dyt, wgu1, wd1, sg, su, sd, dh_out, gg, gu, gd, rawgu, rawd, *scratch):
    h1, dh, a1, acc, scales, dgu, accgu, accd, tsem, lsem, wgu, wd, own, gsems, *refs = scratch
    at = Place()
    grads = (accgu, accd)
    w = Gather(at, (wgu, wd), (sg, su, sd), own, gsems, False)
    red = Reduce(at, grads, refs)
    early = EARLY - C
    loads = [
        [pltpu.make_async_copy(src.at[u], dst.at[u], lsem.at[u, m]) for m, (src, dst) in enumerate(((wgu1, wgu), (wd1, wd)))]
        for u in range(early)
    ]

    def columns(src, dst, k, t):
        return pltpu.make_async_copy(src.at[:, tile(t)], dst.at[:, tile(t)], tsem.at[k, t])

    columns(h1_in, h1, 0, 0).start()
    for copy in loads[0]:
        copy.start()
    for t in range(1, NT):
        columns(h1_in, h1, 0, t).start()
    columns(dyt, dh, 1, 0).start()
    for u in range(early, C):
        w.fetch(u, 1, u)
    for t in range(1, NT):
        columns(dyt, dh, 1, t).start()
    for load in loads[1:]:
        for copy in load:
            copy.start()
    greet((at.core, at.x, at.y, at.z))

    def pre(t, _):
        columns(h1_in, h1, 0, t).wait()
        wide = h1[:, tile(t)].astype(f32)
        scale = scale_of(wide)
        scales[:, tile(t)] = scale
        a1[:, tile(t)] = (wide * scale).astype(bf16)
        acc[:, tile(t)] = jnp.zeros((D, T), f32)
        return 0

    lax.fori_loop(0, NT, pre, 0)
    for u in range(early, C):
        w.send(u)
    for load in loads:
        for copy in load:
            copy.wait()

    outs = (gg, gu, gd)

    def step(i, _):
        c, t = i // NT, i % NT
        slot = c % 2

        @pl.when((t == 0) & (c >= 2))
        def _():
            red.to_zy(c - 2)

        @pl.when((t == 0) & (c >= 1))
        def _():
            red.to_core(c - 1, 1 - slot)

        @pl.when((t == 1) & (c >= 2))
        def _():
            red.last(c - 2, lambda m, value: put_chunk(outs[m], m, c - 2, value))

        @pl.when((t == 1) & (c >= 1))
        def _():
            red.to_x(c - 1, 1 - slot)

        @pl.when((t == 3) & (c >= 1))
        def _():
            red.to_yz(c - 1)

        for u in range(early, C):

            @pl.when(i == 2 * (u - early) + 2)
            def _():
                w.forward(u, 0)
                w.forward(u, 1)

            @pl.when(i == u * NT)
            def _():
                w.ready(u, 0)
                w.ready(u, 1)

        @pl.when(t == 0)
        def _():
            clear(grads, slot)

        @pl.when(i < NT)
        def _():
            columns(dyt, dh, 1, t).wait()

        a = a1[:, tile(t)]
        y = dh[:, tile(t)]
        both = dg(wgu[c], a, 0, 0)
        act, dgu[:F], dgu[F:] = products(both[:F], both[F:], dg(wd[c], y, 1, 0))
        accd[slot] += dg(y, act, 1, 1)
        accgu[slot] += dg(a, dgu[...], 1, 1)
        acc[:, tile(t)] += dg(wgu[c], dgu[...], 1, 0)
        return 0

    lax.fori_loop(0, STEPS, step, 0)
    red.to_zy(C - 2)
    raw = [pltpu.make_async_copy(ref.at[(C - 1) % 2], out, lsem.at[0, m]) for m, (ref, out) in enumerate(zip(grads, (rawgu, rawd)))]
    for copy in raw:
        copy.start()


    def post(t, _):
        scale = scales[:, tile(t)]
        wide = h1[:, tile(t)].astype(f32)
        da = acc[:, tile(t)].astype(bf16).astype(f32)
        along = scale * scale * scale * jnp.mean(da * wide, 0, keepdims=True)
        dh[:, tile(t)] = (dh[:, tile(t)].astype(f32) + (scale * da - along * wide).astype(bf16).astype(f32)).astype(bf16)
        columns(dh, dh_out, 0, t).start()
        return 0

    lax.fori_loop(0, NT, post, 0)
    red.last(C - 2, lambda m, value: put_chunk(outs[m], m, C - 2, value))
    for u in range(early, C):
        w.finish(u)
    for copy in raw:
        copy.wait()
    for t in range(NT):
        columns(dh, dh_out, 0, t).wait()


def squares(value):
    wide = value.astype(f32)
    wide = (wide * wide).reshape(value.shape[0] // 8, 8, value.shape[1]).sum(0)
    return sum(wide[:, n * 128 : (n + 1) * 128] for n in range(value.shape[1] // 128))


def bottom_kernel(a0_in, dh_in, wd_in, gin, uin, rawgu, rawd, gg1, gu1, gd1, gg_out, gu_out, gd_out, total, *scratch):
    a0, dh, wd, gg, gu, gd, accgu, accd, gb, ub, sq, everyone, sems, lsem, nsem, tsem, fsem, *refs = scratch
    at = Place()
    grads = (accgu, accd)
    red = Reduce(at, grads, refs)
    raw = [pltpu.make_async_copy(src, ref.at[1], lsem.at[m]) for m, (ref, src) in enumerate(zip(grads, (rawgu, rawd)))]

    def load(buf, src, k, i):
        return pltpu.make_async_copy(src.at[i // NT, :, tile(i % NT)], buf.at[i % 2], sems.at[k, i % 2])

    def tiles(t):
        return [
            pltpu.make_async_copy(dh_in.at[:, tile(t)], dh.at[:, tile(t)], tsem.at[0, t]),
            pltpu.make_async_copy(a0_in.at[:, tile(t)], a0.at[:, tile(t)], tsem.at[1, t]),
            pltpu.make_async_copy(wd_in.at[t], wd.at[t], tsem.at[2, t]),
        ]

    outs = (gg, gu, gd)
    done = [pltpu.make_async_copy(src, ref.at[1], fsem.at[0, m]) for m, (ref, src) in enumerate(zip(outs, (gg1, gu1, gd1)))]
    for copy in tiles(0):
        copy.start()
    load(gb, gin, 0, 0).start()
    load(ub, uin, 1, 0).start()
    for copy in tiles(1) + raw + tiles(2) + tiles(3) + done:
        copy.start()
    greet((at.core, at.x, at.diag, at.y, at.z))
    sq[...] = jnp.zeros((8, 128), f32)

    def put(u):
        def one(m, value):
            sq[...] += squares(value)
            put_chunk(outs[m].at[jnp.where(u == 0, 1, 0)], m, jnp.where(u == 0, C - 1, u - 1), value)

        return one

    G, U, DOWN = (0,), (1,), (2,)

    def last(u, which):
        red.last(u, put(u), which)

    def step(i, _):
        c, t = i // NT, i % NT
        slot = c % 2

        @pl.when(i < NT)
        def _():
            for copy in tiles(t):
                copy.wait()

        @pl.when(i == 1)
        def _():
            for copy in raw + done:
                copy.wait()

            red.to_core(0, 1)

        @pl.when((t == 0) & (c >= 1))
        def _():
            red.to_core(c, 1 - slot)
            red.to_yz(c - 1, U)

        @pl.when((t == 0) & (c >= 2))
        def _():
            last(c - 2, U)

        @pl.when(t == 0)
        def _():
            clear(grads, slot)

        @pl.when((t == 1) & (c >= 1))
        def _():
            red.to_yz(c - 1, DOWN)
            red.to_zy(c - 1, G)

        @pl.when(((t == 1) & (c >= 1)) | (i == 2))
        def _():
            red.to_x(c, 1 - slot)

        @pl.when((t == 1) & (c >= 2))
        def _():
            last(c - 2, DOWN)

        @pl.when((t == 2) & (c >= 1))
        def _():
            red.to_zy(c - 1, U)

        @pl.when((t == 3) & (c >= 1))
        def _():
            red.to_zy(c - 1, DOWN)
            last(c - 1, G)

        @pl.when(t == 3)
        def _():
            red.to_yz(c, G)

        @pl.when(i + 1 < STEPS)
        def _():
            load(gb, gin, 0, i + 1).start()
            load(ub, uin, 1, i + 1).start()

        load(gb, gin, 0, i).wait()
        load(ub, uin, 1, i).wait()
        a = a0[:, tile(t)]
        y = dh[:, tile(t)]
        da = dg(wd[c], y, 1, 0)
        act, dgate, dup = products(gb[i % 2], ub[i % 2], da)
        accd[slot] += dg(y, act, 1, 1)
        accgu[slot] += dg(a, jnp.concatenate([dgate, dup], 0), 1, 1)
        return 0

    lax.fori_loop(0, STEPS, step, 0)
    red.to_core(C, 1)
    red.to_yz(C - 1, U)
    last(C - 2, U)
    red.to_x(C, 1, G)
    red.to_x(C, 1, U)
    red.to_yz(C - 1, DOWN)
    red.to_x(C, 1, DOWN)
    red.to_zy(C - 1, G)
    last(C - 2, DOWN)
    red.to_zy(C - 1, U)
    for c in range(C - 1):
        for q in range(4):
            sq[...] += squares(gg[1, :, q * F + c * 128 : q * F + (c + 1) * 128]) + squares(gu[1, :, q * F + c * 128 : q * F + (c + 1) * 128])
    sq[...] += squares(gd[1, : (C - 1) * RD, :])
    late = [
        [pltpu.make_async_copy(ref.at[l], out.at[l], fsem.at[1 + l, m]) for m, (ref, out) in enumerate(zip(outs, (gg_out, gu_out, gd_out)))]
        for l in range(2)
    ]
    for copy in late[1]:
        copy.start()
    red.to_zy(C - 1, DOWN)
    red.to_yz(C, G)
    last(C - 1, G)
    last(C - 1, U)
    red.to_yz(C, U)
    red.to_zy(C, G)
    last(C - 1, DOWN)
    red.to_yz(C, DOWN)
    red.to_zy(C, U)
    last(C, G)
    red.to_zy(C, DOWN)
    last(C, U)
    last(C, DOWN)
    for copy in late[0]:
        copy.start()
    everyone[at.s] = sq[...]
    copies = [
        remote(sq, everyone.at[at.s], nsem.at[0, n], nsem.at[1, n], peer) for n, peer in enumerate((at.core, at.x, at.diag))
    ]
    for copy in copies:
        copy.start()
    for copy in copies:
        copy.wait()
    total[...] = everyone[0] + everyone[1] + everyone[2] + everyone[3]
    for copy in late[0] + late[1]:
        copy.wait()


def adamw_kernel(count, total, *refs):
    mean = jnp.sum(total[...], keepdims=True) / count
    factor = jnp.minimum(1.0, 0.5 * lax.rsqrt(mean + 1e-30))
    for n in range(3):
        g, w, m, v, w_out, m_out, v_out = refs[n::3]
        grad = g[...].astype(f32) * factor.reshape(1, 1, 1)
        m_new = 0.9 * m[...] + 0.1 * grad
        v_new = 0.95 * v[...] + 0.05 * grad * grad
        old = w[...].astype(f32)
        w_out[...] = (old - 0.02 * (m_new * lax.rsqrt(v_new + 1e-8) + 0.1 * old)).astype(bf16)
        m_out[...] = m_new
        v_out[...] = v_new


def params(n):
    return pltpu.CompilerParams(vmem_limit_bytes=67_000_000, collective_id=n, has_side_effects=True)


def cost(matmuls):
    return pl.CostEstimate(flops=matmuls * 2 * D * FF * TOK, bytes_accessed=1 << 26, transcendentals=0)


S = jax.ShapeDtypeStruct


def step(x, dy, *arrays):
    shards, m, v = (arrays[i : i + 3] for i in (0, 3, 6))
    early = EARLY - C
    h1, a0, dyt, g, u, wgu1, wd1, wd0 = pl.pallas_call(
        forward_kernel,
        name="forward",
        in_specs=[ANY] * 5,
        out_specs=[ANY] * 8,
        out_shape=[S((D, TOK), bf16)] * 3
        + [S((C, F, TOK), f32)] * 2
        + [S((early, D, 2 * F), bf16), S((early, F, D), bf16), S((C, F, D), bf16)],
        scratch_shapes=[pltpu.VMEM((D, TOK), bf16)] * 2
        + [pltpu.VMEM((D, TOK), f32), pltpu.VMEM((TOK, D), bf16), pltpu.VMEM((D, TOK), bf16)]
        + [pltpu.VMEM((2, F, T), f32), pltpu.VMEM((2, F, T), f32), pltpu.VMEM((2, F, T), bf16), DMA((2, 2))]
        + gather_scratch(EARLY)
        + [DMA((early + 1, 2)), DMA((NT,)), DMA((3, NT))],
        compiler_params=params(0),
        cost_estimate=cost(3),
    )(x[0], dy[0], *shards)
    dh, gg1, gu1, gd1, *raw = pl.pallas_call(
        top_kernel,
        name="top",
        in_specs=[ANY] * 7,
        out_specs=[ANY] + [VMEM] * 3 + [ANY] * 2,
        out_shape=[S((D, TOK), bf16), S((RG, FF), bf16), S((RG, FF), bf16), S((C * RD, D), bf16)] + [S((D, 2 * F), f32), S((D, F), f32)],
        scratch_shapes=[
            pltpu.VMEM((D, TOK), bf16),
            pltpu.VMEM((D, TOK), bf16),
            pltpu.VMEM((D, TOK), bf16),
            pltpu.VMEM((D, TOK), f32),
            pltpu.VMEM((1, TOK), f32),
            pltpu.VMEM((2 * F, T), bf16),
            pltpu.VMEM((2, D, 2 * F), f32),
            pltpu.VMEM((2, D, F), f32),
        ]
        + [DMA((2, NT)), DMA((C, 2))]
        + gather_scratch(C)
        + reduce_scratch(),
        compiler_params=params(1),
        cost_estimate=cost(8),
    )(h1, dyt, wgu1, wd1, *shards)
    *grads, total = pl.pallas_call(
        bottom_kernel,
        name="bottom",
        in_specs=[ANY] * 10,
        out_specs=[ANY] * 3 + [VMEM],
        out_shape=[S((2, RG, FF), bf16), S((2, RG, FF), bf16), S((2, C * RD, D), bf16), S((8, 128), f32)],
        scratch_shapes=[
            pltpu.VMEM((D, TOK), bf16),
            pltpu.VMEM((D, TOK), bf16),
            pltpu.VMEM((C, F, D), bf16),
            pltpu.VMEM((2, RG, FF), bf16),
            pltpu.VMEM((2, RG, FF), bf16),
            pltpu.VMEM((2, C * RD, D), bf16),
            pltpu.VMEM((2, D, 2 * F), f32),
            pltpu.VMEM((2, D, F), f32),
            pltpu.VMEM((2, F, T), f32),
            pltpu.VMEM((2, F, T), f32),
            pltpu.VMEM((8, 128), f32),
            pltpu.VMEM((4, 8, 128), f32),
            DMA((2, 2)),
            DMA((2,)),
            DMA((2, 3)),
            DMA((3, NT)),
            DMA((3, 3)),
        ]
        + reduce_scratch(),
        compiler_params=params(2),
        cost_estimate=cost(4),
    )(a0, dh, wd0, g, u, *raw, gg1, gu1, gd1)
    blocks = [pl.BlockSpec((1, w.shape[1] // 2, w.shape[2]), lambda l, i: (l, i, 0)) for w in shards]
    count = 4 * sum(w.size for w in shards)
    return pl.pallas_call(
        lambda *refs: adamw_kernel(count, *refs),
        name="adamw",
        grid=(2, 2),
        in_specs=[pl.BlockSpec((8, 128), lambda l, i: (0, 0))] + blocks * 4,
        out_specs=blocks * 3,
        out_shape=[S(w.shape, bf16) for w in shards] + [S(w.shape, f32) for w in shards] * 2,
        compiler_params=pltpu.CompilerParams(vmem_limit_bytes=60_000_000),
        cost_estimate=pl.CostEstimate(flops=40 << 20, bytes_accessed=43 << 20, transcendentals=0),
    )(total, *grads, *shards, *m, *v)


def solution(mesh):
    states, cut = P(("rep", "r", "s"), None, None), P(None, "s", None)
    return jax.shard_map(
        step,
        mesh=mesh,
        in_specs=(states, states) + (cut,) * 9,
        out_specs=(P("rep", "s", None),) * 9,
        check_vma=False,
    )
```
